16 devices in a mesh: pool: 16 (over z, y, x, core).
Axes of the slice: x: 2, y: 2, z: 2, core: 2. Of those that a mesh axis runs over, the one named last changes fastest.
Arguments:
- hidden: bfloat16 [16, 64, 2048], P('pool')
- prefix_len: int32 [16], P('pool')
- prefix_table: int32 [16, 256, 2], P('pool')
- write_table: int32 [16, 1, 2], P('pool')
- cache_c: bfloat16 [16, 65, 64, 512], P('pool')
- cache_kr: bfloat16 [16, 65, 64, 64], P('pool')
- w_q: bfloat16 [2048, 3072], replicated
- w_dkv: bfloat16 [2048, 576], replicated
- g_kv: bfloat16 [512], replicated
- w_uk: bfloat16 [512, 16, 128], replicated
- w_uv: bfloat16 [512, 16, 128], replicated
- w_o: bfloat16 [2048, 2048], replicated
Outputs:
- output 1: bfloat16 [16, 64, 2048], P('pool')
- output 2: bfloat16 [16, 65, 64, 512], P('pool')
- output 3: bfloat16 [16, 65, 64, 64], P('pool')
All inputs are finite; a program needn't handle non-finite values.
Results may differ from the reference program's by a relative error of at most 0.00655557.
Values are sent between devices in bfloat16 or wider.
A program may use at most 1 GiB of HBM per device.

```python
import math
import jax
import jax.numpy as jnp
from jax import lax

POOL_SIZE = 16
REQ_DEV = 1
CHUNK_LEN = 64
PREFIX_MAX = 16384
PREFIX_PAGES = 64
D_MODEL = 2048
NUM_HEADS = 16
PAGE_LEN = 64
LATENT = 512
ROPE_DIM = 64
NOPE_DIM = 128
VALUE_DIM = 128

REQUESTS = POOL_SIZE * REQ_DEV
TABLE_PAGES = PREFIX_MAX // PAGE_LEN
CHUNK_PAGES = CHUNK_LEN // PAGE_LEN
CACHE_PAGES = PREFIX_PAGES + REQ_DEV * CHUNK_PAGES
READ_SLOTS = max(1, (2 * REQ_DEV * TABLE_PAGES) // POOL_SIZE)
NORM_EPS = 1e-6
ROPE_BASE = 10000.0


def rope_tables(positions):
    half_dim = ROPE_DIM // 2
    inv_freq = ROPE_BASE ** (-jnp.arange(half_dim, dtype=jnp.float32) / half_dim)
    angles = positions.astype(jnp.float32)[..., None] * inv_freq
    return jnp.cos(angles), jnp.sin(angles)


def apply_rope(values, cos_tab, sin_tab):
    half_dim = ROPE_DIM // 2
    first = values[..., :half_dim]
    second = values[..., half_dim:]
    return jnp.concatenate([first * cos_tab - second * sin_tab, second * cos_tab + first * sin_tab], axis=-1)


def draw_tables(key):
    key_len, key_perm, key_rot, key_page, key_write = jax.random.split(key, 5)
    req_ids = jnp.arange(REQUESTS)
    page_counts = jax.random.randint(key_len, (REQUESTS,), 0, TABLE_PAGES + 1)
    page_counts = jnp.where(req_ids == 0, TABLE_PAGES, jnp.where(req_ids == REQUESTS - 1, 0, page_counts))
    prefix_len = (page_counts * PAGE_LEN).astype(jnp.int32)
    is_valid = (jnp.arange(TABLE_PAGES)[None, :] < page_counts[:, None]).reshape(POOL_SIZE, REQ_DEV * TABLE_PAGES)
    slot_rank = jnp.cumsum(is_valid.astype(jnp.int32), axis=1) - 1
    owner_perm = jax.random.permutation(key_perm, POOL_SIZE)
    rotation = jax.random.randint(key_rot, (POOL_SIZE, 1), 0, max(1, POOL_SIZE // 4))
    owners = owner_perm[(rotation + slot_rank // READ_SLOTS) % POOL_SIZE]
    page_pick = jax.random.randint(key_page, (POOL_SIZE, REQ_DEV * TABLE_PAGES), 0, PREFIX_PAGES)
    prefix_table = jnp.stack([jnp.where(is_valid, owners, -1), jnp.where(is_valid, page_pick, -1)], axis=-1)
    prefix_table = prefix_table.reshape(REQUESTS, TABLE_PAGES, 2).astype(jnp.int32)
    write_ids = jnp.arange(REQ_DEV * CHUNK_PAGES)
    offsets = jax.random.permutation(key_write, POOL_SIZE)[write_ids % POOL_SIZE]
    write_owner = (jnp.arange(POOL_SIZE)[:, None] + offsets[None, :]) % POOL_SIZE
    write_page = jnp.broadcast_to(PREFIX_PAGES + write_ids[None, :], (POOL_SIZE, REQ_DEV * CHUNK_PAGES))
    write_table = jnp.stack([write_owner, write_page], axis=-1).reshape(REQUESTS, CHUNK_PAGES, 2).astype(jnp.int32)
    return prefix_len, prefix_table, write_table


def setup_inputs(seed: int = 0) -> dict:
    key_list = jax.random.split(jax.random.key(seed), 12)
    prefix_len, prefix_table, write_table = draw_tables(key_list[0])
    q_gain = math.sqrt(math.log((PREFIX_MAX + CHUNK_LEN) / 8.0) / 3.0)
    hidden = jax.random.normal(key_list[1], (REQUESTS, CHUNK_LEN, D_MODEL), jnp.float32)
    cache_c = jax.random.normal(key_list[2], (POOL_SIZE, CACHE_PAGES, PAGE_LEN, LATENT), jnp.float32)
    cache_kr = jax.random.normal(key_list[3], (POOL_SIZE, CACHE_PAGES, PAGE_LEN, ROPE_DIM), jnp.float32)
    w_q = jax.random.normal(key_list[4], (D_MODEL, NUM_HEADS * (NOPE_DIM + ROPE_DIM)), jnp.float32) * (q_gain / math.sqrt(D_MODEL))
    w_dkv = jax.random.normal(key_list[5], (D_MODEL, LATENT + ROPE_DIM), jnp.float32) / math.sqrt(D_MODEL)
    g_kv = jax.random.uniform(key_list[6], (LATENT,), jnp.float32, 0.5, 1.5)
    w_uk = jax.random.normal(key_list[7], (LATENT, NUM_HEADS, NOPE_DIM), jnp.float32) / math.sqrt(NOPE_DIM)
    w_uv = jax.random.normal(key_list[8], (LATENT, NUM_HEADS, VALUE_DIM), jnp.float32) / math.sqrt(LATENT)
    w_o = jax.random.normal(key_list[9], (NUM_HEADS * VALUE_DIM, D_MODEL), jnp.float32) / math.sqrt(NUM_HEADS * VALUE_DIM)
    return {
        "hidden": hidden.astype(jnp.bfloat16),
        "prefix_len": prefix_len,
        "prefix_table": prefix_table,
        "write_table": write_table,
        "cache_c": cache_c.astype(jnp.bfloat16),
        "cache_kr": cache_kr.astype(jnp.bfloat16),
        "w_q": w_q.astype(jnp.bfloat16),
        "w_dkv": w_dkv.astype(jnp.bfloat16),
        "g_kv": g_kv.astype(jnp.bfloat16),
        "w_uk": w_uk.astype(jnp.bfloat16),
        "w_uv": w_uv.astype(jnp.bfloat16),
        "w_o": w_o.astype(jnp.bfloat16),
    }


def reference(hidden, prefix_len, prefix_table, write_table, cache_c, cache_kr, w_q, w_dkv, g_kv, w_uk, w_uv, w_o):
    flat_c = cache_c.reshape(POOL_SIZE * CACHE_PAGES, PAGE_LEN, LATENT)
    flat_kr = cache_kr.reshape(POOL_SIZE * CACHE_PAGES, PAGE_LEN, ROPE_DIM)
    score_scale = (NOPE_DIM + ROPE_DIM) ** -0.5
    w_uk32 = w_uk.astype(jnp.float32)
    w_uv32 = w_uv.astype(jnp.float32)
    kv_gain = g_kv.astype(jnp.float32)
    query_ids = jnp.arange(CHUNK_LEN)
    key_ids = jnp.arange(PREFIX_MAX + CHUNK_LEN)

    def one_request(req_item):
        x_req, pre_len, req_table = req_item
        page_ids = jnp.maximum(req_table[:, 0], 0) * CACHE_PAGES + jnp.maximum(req_table[:, 1], 0)
        pre_c = flat_c[page_ids].reshape(PREFIX_MAX, LATENT)
        pre_kr = flat_kr[page_ids].reshape(PREFIX_MAX, ROPE_DIM)
        q_all = jnp.dot(x_req, w_q, preferred_element_type=jnp.float32).astype(jnp.bfloat16)
        q_all = q_all.reshape(CHUNK_LEN, NUM_HEADS, NOPE_DIM + ROPE_DIM)
        kv_lat = jnp.dot(x_req, w_dkv, preferred_element_type=jnp.float32)
        lat_part = kv_lat[:, :LATENT]
        inv_rms = lax.rsqrt(jnp.mean(lat_part * lat_part, axis=-1, keepdims=True) + NORM_EPS)
        c_new = (lat_part * inv_rms * kv_gain).astype(jnp.bfloat16)
        cos_tab, sin_tab = rope_tables(pre_len + query_ids)
        kr_new = apply_rope(kv_lat[:, LATENT:], cos_tab, sin_tab).astype(jnp.bfloat16)
        q_rope = apply_rope(q_all[:, :, NOPE_DIM:].astype(jnp.float32), cos_tab[:, None, :], sin_tab[:, None, :]).astype(jnp.bfloat16)
        q_lat = jnp.einsum("chn,lhn->chl", q_all[:, :, :NOPE_DIM].astype(jnp.float32), w_uk32).astype(jnp.bfloat16)
        keys_c = jnp.concatenate([pre_c, c_new], axis=0).astype(jnp.float32)
        keys_r = jnp.concatenate([pre_kr, kr_new], axis=0).astype(jnp.float32)
        scores = jnp.einsum("chl,jl->hcj", q_lat.astype(jnp.float32), keys_c)
        scores = (scores + jnp.einsum("chr,jr->hcj", q_rope.astype(jnp.float32), keys_r)) * score_scale
        visible = jnp.where(key_ids[None, :] < PREFIX_MAX, key_ids[None, :] < pre_len, key_ids[None, :] - PREFIX_MAX <= query_ids[:, None])
        scores = jnp.where(visible[None, :, :], scores, -jnp.inf)
        weights = jax.nn.softmax(scores, axis=-1)
        o_lat = jnp.einsum("hcj,jl->chl", weights, keys_c).astype(jnp.bfloat16)
        o_heads = jnp.einsum("chl,lhv->chv", o_lat.astype(jnp.float32), w_uv32).astype(jnp.bfloat16)
        attn_out = jnp.dot(o_heads.reshape(CHUNK_LEN, NUM_HEADS * VALUE_DIM), w_o, preferred_element_type=jnp.float32)
        y_req = (x_req.astype(jnp.float32) + attn_out).astype(jnp.bfloat16)
        return y_req, c_new, kr_new

    hidden_out, new_c, new_kr = lax.map(one_request, (hidden, prefix_len, prefix_table))
    dest_rows = (write_table[:, :, 0] * CACHE_PAGES + write_table[:, :, 1]).reshape(REQUESTS * CHUNK_PAGES)
    cache_c_out = flat_c.at[dest_rows].set(new_c.reshape(REQUESTS * CHUNK_PAGES, PAGE_LEN, LATENT))
    cache_kr_out = flat_kr.at[dest_rows].set(new_kr.reshape(REQUESTS * CHUNK_PAGES, PAGE_LEN, ROPE_DIM))
    cache_c_out = cache_c_out.reshape(POOL_SIZE, CACHE_PAGES, PAGE_LEN, LATENT)
    cache_kr_out = cache_kr_out.reshape(POOL_SIZE, CACHE_PAGES, PAGE_LEN, ROPE_DIM)
    return hidden_out, cache_c_out, cache_kr_out
```

```python
import functools
import math

import jax
import jax.numpy as jnp
import numpy as np
from jax import lax
from jax.experimental import pallas as pl
from jax.experimental.pallas import tpu as pltpu
from jax.sharding import PartitionSpec as P

MESH = pl.DeviceIdType.MESH
BF16 = jnp.bfloat16
F32 = jnp.float32

CHIPS = 8
DEVS = 16
TOK = 64
D_MODEL = 2048
HALF = 8
PAGE = 64
LAT = 512
ROPE = 64
NOPE = 128
KEYW = 640
ROWS = HALF * TOK
TABLE = 256
SLOTS = 64
OUTR = ROWS + 8
NORM_EPS = 1e-6
ROPE_BASE = 10000.0
EXP_SCALE = (NOPE + ROPE) ** -0.5 * math.log2(math.e)
NEG = -1e30
BLK_PAGES = 8
BLK = BLK_PAGES * PAGE


def xor3(a, b, bits):
    out = 0
    for i in range(bits):
        x = lax.rem(lax.div(a, 2**i), 2)
        y = lax.rem(lax.div(b, 2**i), 2) if not isinstance(b, int) else (b >> i) % 2
        out = out + 2**i * (x + y - 2 * x * y)
    return out


def project_kernel(
    x_hbm, meta_hbm, cos_ref, sin_ref, gkv_ref, wq_hbm, wdkv_hbm, wuk_hbm, cc_hbm, ckr_hbm,
    u_hbm, nk_hbm, list_ref, pc_hbm, pkr_hbm,
    xall, metas, wq, wdkv, wuk, ubuf, nkbuf,
    loc_sem, xs_sem, xr_sem, fs_sem, fr_sem, ms_sem, mr_sem, cs_sem, cr_sem, us_sem, ns_sem,
):
    me = lax.axis_index("pool")
    chip = lax.div(me, 2)
    core = lax.rem(me, 2)
    partner = me + 1 - 2 * core
    my_rows = pl.ds(pl.multiple_of(core * TOK, TOK), TOK)
    pt_rows = pl.ds(pl.multiple_of((1 - core) * TOK, TOK), TOK)

    x_in = pltpu.make_async_copy(x_hbm.at[0], xall.at[chip, my_rows], loc_sem.at[0])
    x_in.start()
    m_in = pltpu.make_async_copy(meta_hbm, metas.at[me], loc_sem.at[1])
    m_in.start()
    wq_in = [
        pltpu.make_async_copy(
            wq_hbm.at[:, pl.ds(pl.multiple_of(core * (HALF * 192) + j * 384, 128), 384)],
            wq.at[j], loc_sem.at[2 + j])
        for j in range(4)
    ]
    wuk_in = pltpu.make_async_copy(wuk_hbm.at[pl.ds(core * HALF, HALF)], wuk, loc_sem.at[6])
    wdkv_in = pltpu.make_async_copy(wdkv_hbm, wdkv, loc_sem.at[7])
    wdkv_in.start()
    for c in wq_in:
        c.start()
    wuk_in.start()

    barrier = pltpu.get_barrier_semaphore()
    for e in range(1, DEVS):
        pl.semaphore_signal(barrier, inc=1, device_id=(xor3(me, e, 4),), device_id_type=MESH)
    x_in.wait()
    m_in.wait()
    pl.semaphore_wait(barrier, DEVS - 1)

    x_own = xall.at[chip, my_rows]
    sends = []
    for e in range(1, DEVS):
        sends.append(pltpu.make_async_remote_copy(
            src_ref=metas.at[me], dst_ref=metas.at[me], send_sem=ms_sem.at[e], recv_sem=mr_sem.at[e],
            device_id=(xor3(me, e, 4),), device_id_type=MESH))
    sends.append(pltpu.make_async_remote_copy(
        src_ref=x_own, dst_ref=x_own, send_sem=fs_sem.at[0], recv_sem=fr_sem.at[0],
        device_id=(partner,), device_id_type=MESH))
    for d in range(1, CHIPS):
        sends.append(pltpu.make_async_remote_copy(
            src_ref=x_own, dst_ref=x_own, send_sem=xs_sem.at[d], recv_sem=xr_sem.at[d],
            device_id=(2 * xor3(chip, d, 3) + core,), device_id_type=MESH))
    pc = pltpu.make_async_remote_copy(
        src_ref=cc_hbm.at[0, pl.ds(0, PAGE)], dst_ref=pc_hbm, send_sem=cs_sem.at[0], recv_sem=cr_sem.at[0],
        device_id=(partner,), device_id_type=MESH)
    pkr = pltpu.make_async_remote_copy(
        src_ref=ckr_hbm.at[0, pl.ds(0, PAGE)], dst_ref=pkr_hbm, send_sem=cs_sem.at[1], recv_sem=cr_sem.at[1],
        device_id=(partner,), device_id_type=MESH)
    sends += [pc, pkr]
    for s in sends:
        s.start()

    for e in range(1, DEVS):
        src = xor3(me, e, 4)
        pltpu.make_async_remote_copy(
            src_ref=metas.at[src], dst_ref=metas.at[src], send_sem=ms_sem.at[e], recv_sem=mr_sem.at[e],
            device_id=(src,), device_id_type=MESH).wait_recv()
    own = jnp.concatenate([metas[:, 0, :], metas[:, 1, :]], axis=1)
    page = jnp.concatenate([metas[:, 2, :], metas[:, 3, :]], axis=1)
    first = (2 * chip).astype(F32)
    mask = jnp.where(own >= first, 1.0, 0.0) * jnp.where(own < first + 2.0, 1.0, 0.0)
    tri_r = lax.broadcasted_iota(jnp.int32, (TABLE, TABLE), 0)
    tri_c = lax.broadcasted_iota(jnp.int32, (TABLE, TABLE), 1)
    tri = jnp.where(tri_r < tri_c, 1.0, 0.0).astype(BF16)
    rank = jnp.dot(mask.astype(BF16), tri, preferred_element_type=F32)
    rank = jnp.where(mask > 0.5, rank, -1.0)
    local = (own - first) * float(PAGE) + page
    lane = lax.broadcasted_iota(jnp.int32, (DEVS, 128), 1)
    count = jnp.sum(mask, axis=1, keepdims=True)
    req_id = lax.broadcasted_iota(jnp.int32, (DEVS, 1), 0).astype(F32)
    wr = jnp.sum(jnp.where(metas[:, 5, 0:1] == me.astype(F32), req_id, 0.0), axis=0, keepdims=True)
    base = jnp.where(lane == SLOTS, count, jnp.where(lane == SLOTS + 1, wr, 0.0))

    def slot(s, acc):
        hit = jnp.sum(jnp.where(rank == s.astype(F32), local, 0.0), axis=1, keepdims=True)
        return jnp.where(lane == s, hit, acc)

    list_ref[...] = lax.fori_loop(0, SLOTS, slot, base).astype(jnp.int32)

    lane2 = lax.broadcasted_iota(jnp.int32, (1, 128), 1)
    low = lane2 < 64
    first_half = lax.rem(lane2, 64) < 32
    wdkv_in.wait()
    for c in wq_in:
        c.wait()
    wuk_in.wait()

    def rotate(v, cos_t, sin_t):
        turned = jnp.where(first_half, pltpu.roll(v, 96, 1), pltpu.roll(v, 32, 1))
        return v * cos_t + turned * sin_t

    def fwd(d, src_chip, rows):
        ref = xall.at[src_chip, rows]
        return pltpu.make_async_remote_copy(
            src_ref=ref, dst_ref=ref, send_sem=fs_sem.at[d], recv_sem=fr_sem.at[d],
            device_id=(partner,), device_id_type=MESH)

    def out_copies(slot_id, src_chip):
        return (pltpu.make_async_copy(ubuf.at[slot_id], u_hbm.at[src_chip], us_sem.at[slot_id]),
                pltpu.make_async_copy(nkbuf.at[slot_id], nk_hbm.at[src_chip], ns_sem.at[slot_id]))

    def step(d, carry):
        src_chip = xor3(chip, d, 3)
        slot_id = lax.rem(d, 2)

        @pl.when(d > 0)
        def _():
            ref = xall.at[src_chip, my_rows]
            pltpu.make_async_remote_copy(
                src_ref=ref, dst_ref=ref, send_sem=xs_sem.at[d], recv_sem=xr_sem.at[d],
                device_id=(partner,), device_id_type=MESH).wait_recv()
            fwd(d, src_chip, my_rows).start()

        fwd(d, src_chip, pt_rows).wait_recv()

        @pl.when(d > 1)
        def _():
            for c in out_copies(slot_id, src_chip):
                c.wait()

        cs, ss = [], []
        for half in range(2):
            b = metas[2 * src_chip + half, 4:5, :]
            br = pltpu.roll(b, 64, 1)
            cp = jnp.where(low, b, br)
            sp = jnp.where(low, br, b)
            cs.append(cp * cos_ref[...] - sp * sin_ref[...])
            ss.append((sp * cos_ref[...] + cp * sin_ref[...]) * jnp.where(first_half, -1.0, 1.0))
        cos_t = jnp.concatenate(cs, axis=0)
        sin_t = jnp.concatenate(ss, axis=0)

        kv = jnp.dot(xall[src_chip], wdkv[...], preferred_element_type=F32)
        lat = kv[:, :LAT]
        inv = lax.rsqrt(jnp.mean(lat * lat, axis=-1, keepdims=True) + NORM_EPS)
        c_new = (lat * inv * gkv_ref[...].astype(F32)).astype(BF16)
        kr = jnp.concatenate([kv[:, LAT:], jnp.zeros((2 * TOK, 64), F32)], axis=1)
        kr = rotate(kr, cos_t, sin_t).astype(BF16)
        for half in range(2):
            rows = slice(half * TOK, (half + 1) * TOK)
            nkbuf[slot_id, half, :, :LAT] = c_new[rows]
            nkbuf[slot_id, half, :, LAT:] = kr[rows]

        def pair(j, carry):
            q = jnp.dot(xall[src_chip], wq[j], preferred_element_type=F32).astype(BF16)
            nope = (q[:, 0:128], jnp.concatenate([q[:, 192:256], q[:, 256:320]], axis=1))
            rp = jnp.concatenate([q[:, 128:192], q[:, 320:384]], axis=1).astype(F32)
            rp = rotate(rp, cos_t, sin_t)
            rps = (jnp.where(low, rp, 0.0).astype(BF16), jnp.where(low, pltpu.roll(rp, 64, 1), 0.0).astype(BF16))
            for i in range(2):
                u = jnp.dot(nope[i], wuk[2 * j + i], preferred_element_type=F32).astype(BF16)
                head_rows = pl.ds(pl.multiple_of((2 * j + i) * TOK, TOK), TOK)
                for half in range(2):
                    rows = slice(half * TOK, (half + 1) * TOK)
                    ubuf[slot_id, half, head_rows, :LAT] = u[rows]
                    ubuf[slot_id, half, head_rows, LAT:] = rps[i][rows]
            return carry

        lax.fori_loop(0, 4, pair, 0)
        for c in out_copies(slot_id, src_chip):
            c.start()
        return carry

    lax.fori_loop(0, CHIPS, step, 0)
    for slot_id in range(2):
        for c in out_copies(slot_id, chip):
            c.wait()
    for s in sends[:-2]:
        s.wait_send()
    for d in range(1, CHIPS):
        fwd(d, chip, my_rows).wait_send()
    pc.wait()
    pkr.wait()


def project(x, meta, cos_i, sin_i, g_kv, w_q, w_dkv, w_ukt, cache_c, cache_kr):
    any_spec = pl.BlockSpec(memory_space=pl.ANY)
    vmem = pl.BlockSpec(memory_space=pltpu.VMEM)
    dma = pltpu.SemaphoreType.DMA
    return pl.pallas_call(
        project_kernel,
        out_shape=(
            jax.ShapeDtypeStruct((CHIPS, 2, ROWS, KEYW), BF16),
            jax.ShapeDtypeStruct((CHIPS, 2, TOK, KEYW), BF16),
            jax.ShapeDtypeStruct((DEVS, 128), jnp.int32),
            jax.ShapeDtypeStruct((PAGE, PAGE, LAT), BF16),
            jax.ShapeDtypeStruct((PAGE, PAGE, ROPE), BF16),
        ),
        in_specs=[any_spec, any_spec, vmem, vmem, vmem, any_spec, any_spec, any_spec, any_spec, any_spec],
        out_specs=(any_spec, any_spec, vmem, any_spec, any_spec),
        scratch_shapes=[
            pltpu.VMEM((CHIPS, 2 * TOK, D_MODEL), BF16),
            pltpu.VMEM((DEVS, 8, 128), F32),
            pltpu.VMEM((4, D_MODEL, 384), BF16),
            pltpu.VMEM((D_MODEL, LAT + ROPE), BF16),
            pltpu.VMEM((HALF, NOPE, LAT), BF16),
            pltpu.VMEM((2, 2, ROWS, KEYW), BF16),
            pltpu.VMEM((2, 2, TOK, KEYW), BF16),
            dma((8,)), dma((8,)), dma((8,)), dma((8,)), dma((8,)), dma((16,)), dma((16,)),
            dma((2,)), dma((2,)), dma((2,)), dma((2,)),
        ],
        compiler_params=pltpu.CompilerParams(collective_id=0, has_side_effects=True, vmem_limit_bytes=48 * 2**20),
        name="project",
    )(x, meta, cos_i, sin_i, g_kv, w_q, w_dkv, w_ukt, cache_c, cache_kr)


def to_rows(col):
    lane = lax.broadcasted_iota(jnp.int32, (128, 128), 1)
    row = lax.broadcasted_iota(jnp.int32, (128, 128), 0)
    parts = [jnp.sum(jnp.where(lane == row, col[i * 128:(i + 1) * 128], 0.0), axis=0, keepdims=True) for i in range(4)]
    return jnp.concatenate(parts, axis=0)


def attend_kernel(
    list_ref, order_ref,
    u_ref, nk_hbm, wuv_ref, cc_hbm, ckr_hbm, pc_hbm, pkr_hbm,
    out_ref, occ_hbm, ockr_hbm,
    kv, krs, kblk, acc, m_s, l_s, nk_own, nk_wr, sem, osem,
):
    g = pl.program_id(0)
    core = order_ref[8]
    chip = order_ref[9]
    src_chip = order_ref[g]
    own = pl.ds(pl.multiple_of(core * PAGE, PAGE), PAGE)
    oth = pl.ds(pl.multiple_of((1 - core) * PAGE, PAGE), PAGE)
    wr = list_ref[0, SLOTS + 1]

    outs = (
        pltpu.make_async_copy(kv.at[own, :, pl.ds(0, LAT)], occ_hbm.at[0, pl.ds(0, PAGE)], osem.at[0]),
        pltpu.make_async_copy(krs.at[own], ockr_hbm.at[0, pl.ds(0, PAGE)], osem.at[1]),
        pltpu.make_async_copy(nk_wr.at[:, pl.ds(0, LAT)], occ_hbm.at[0, PAGE], osem.at[2]),
        pltpu.make_async_copy(krs.at[2 * PAGE], ockr_hbm.at[0, PAGE], osem.at[3]),
    )

    @pl.when(g == 0)
    def _():
        ins = (
            pltpu.make_async_copy(ckr_hbm.at[0, pl.ds(0, PAGE)], krs.at[own], sem.at[0]),
            pltpu.make_async_copy(pkr_hbm, krs.at[oth], sem.at[1]),
            pltpu.make_async_copy(nk_hbm.at[lax.div(wr, 2), lax.rem(wr, 2)], nk_wr, sem.at[2]),
            pltpu.make_async_copy(nk_hbm.at[chip], nk_own, sem.at[3]),
            pltpu.make_async_copy(cc_hbm.at[0, pl.ds(0, PAGE)], kv.at[own, :, pl.ds(0, LAT)], sem.at[4]),
            pltpu.make_async_copy(pc_hbm, kv.at[oth, :, pl.ds(0, LAT)], sem.at[5]),
        )
        for c in ins:
            c.start()
        for c in ins[:4]:
            c.wait()

        def fill(p, carry):
            kv[p, :, LAT:] = jnp.concatenate([krs[p], jnp.zeros((PAGE, 64), BF16)], axis=1)
            return carry

        lax.fori_loop(0, 2 * PAGE, fill, 0)
        krs[2 * PAGE] = nk_wr[:, LAT:LAT + ROPE]
        for c in ins[4:]:
            c.wait()
        for c in outs:
            c.start()

    def update(r, keys, bias):
        s = lax.dot_general(u_ref[0, r], keys, (((1,), (1,)), ((), ())), preferred_element_type=F32)
        s = s + bias
        m_old = m_s[:, 0:1]
        m_new = jnp.maximum(m_old, jnp.max(s, axis=1, keepdims=True))
        alpha = jnp.exp2((m_old - m_new) * EXP_SCALE)
        p = jnp.exp2((s - m_new) * EXP_SCALE)
        width = s.shape[1]
        if width >= 128:
            part = p[:, 0:128]
            for i in range(1, width // 128):
                part = part + p[:, i * 128:(i + 1) * 128]
        else:
            part = jnp.concatenate([p, jnp.zeros((ROWS, 128 - width), F32)], axis=1)
        l_s[...] = l_s[...] * alpha + part
        m_s[...] = jnp.broadcast_to(m_new, m_s.shape)
        acc[...] = acc[...] * alpha + jnp.dot(p.astype(BF16), keys[:, :LAT], preferred_element_type=F32)

    for r in range(2):
        req = 2 * src_chip + r
        n = list_ref[req, SLOTS]
        acc[...] = jnp.zeros_like(acc)
        l_s[...] = jnp.zeros_like(l_s)
        m_s[...] = jnp.full_like(m_s, NEG)

        def block(b, carry):
            for j in range(BLK_PAGES):
                kblk[j * PAGE:(j + 1) * PAGE, :] = kv[list_ref[req, b * BLK_PAGES + j]]
            key = b * BLK + lax.broadcasted_iota(jnp.int32, (1, BLK), 1)
            update(r, kblk[...], jnp.where(key < n * PAGE, 0.0, -jnp.inf))
            return carry

        lax.fori_loop(0, lax.div(n + BLK_PAGES - 1, BLK_PAGES), block, 0)

        @pl.when(src_chip == chip)
        def _():
            row = lax.rem(lax.broadcasted_iota(jnp.int32, (ROWS, TOK), 0), TOK)
            key = lax.broadcasted_iota(jnp.int32, (ROWS, TOK), 1)
            update(r, nk_own[r], jnp.where(key <= row, 0.0, -jnp.inf))

        out_ref[0, r, ROWS:ROWS + 4, :] = to_rows(m_s[:, 0:1])
        out_ref[0, r, ROWS + 4:, :] = to_rows(jnp.sum(l_s[...], axis=1, keepdims=True))
        for h in range(HALF):
            rows = slice(h * TOK, (h + 1) * TOK)
            a = acc[rows, :]
            hi = a.astype(BF16)
            lo = (a - hi.astype(F32)).astype(BF16)
            both = jnp.dot(jnp.concatenate([hi, lo], axis=0), wuv_ref[h], preferred_element_type=F32)
            out_ref[0, r, rows, :] = both[:TOK] + both[TOK:]

    @pl.when(g == CHIPS - 1)
    def _():
        for c in outs:
            c.wait()


def attend(lists, order, u, nk, w_uvt, cache_c, cache_kr, peer_c, peer_kr):
    any_spec = pl.BlockSpec(memory_space=pl.ANY)
    dma = pltpu.SemaphoreType.DMA
    return pl.pallas_call(
        attend_kernel,
        grid_spec=pltpu.PrefetchScalarGridSpec(
            num_scalar_prefetch=2,
            grid=(CHIPS,),
            in_specs=[
                pl.BlockSpec((1, 2, ROWS, KEYW), lambda g, l, o: (o[g], 0, 0, 0)),
                any_spec,
                pl.BlockSpec((HALF, LAT, NOPE), lambda g, l, o: (o[8], 0, 0)),
                any_spec, any_spec, any_spec, any_spec,
            ],
            out_specs=(
                pl.BlockSpec((1, 2, OUTR, 128), lambda g, l, o: (o[g], 0, 0, 0)),
                any_spec, any_spec,
            ),
            scratch_shapes=[
                pltpu.VMEM((2 * PAGE, PAGE, KEYW), BF16),
                pltpu.VMEM((2 * PAGE + 1, PAGE, ROPE), BF16),
                pltpu.VMEM((BLK, KEYW), BF16),
                pltpu.VMEM((ROWS, LAT), F32),
                pltpu.VMEM((ROWS, 128), F32),
                pltpu.VMEM((ROWS, 128), F32),
                pltpu.VMEM((2, TOK, KEYW), BF16),
                pltpu.VMEM((TOK, KEYW), BF16),
                dma((6,)), dma((4,)),
            ],
        ),
        out_shape=(
            jax.ShapeDtypeStruct((CHIPS, 2, OUTR, 128), F32),
            jax.ShapeDtypeStruct(cache_c.shape, BF16),
            jax.ShapeDtypeStruct(cache_kr.shape, BF16),
        ),
        compiler_params=pltpu.CompilerParams(vmem_limit_bytes=56 * 2**20),
        name="attend",
    )(lists, order, u, nk, w_uvt, cache_c, cache_kr, peer_c, peer_kr)


def solution(mesh):
    tok_ids = np.arange(TOK, dtype=np.float64)[:, None]
    inv_freq = ROPE_BASE ** (-np.arange(32, dtype=np.float64) / 32)
    cos_i = np.tile(np.cos(tok_ids * inv_freq), (1, 4)).astype(np.float32)
    sin_i = np.tile(np.sin(tok_ids * inv_freq), (1, 4)).astype(np.float32)

    def device_step(hidden, pre_len, pre_table, wr_table, cache_c, cache_kr, w_q, w_dkv, g_kv, w_uk, w_uv, w_o):
        me = lax.axis_index("pool")
        chip = me // 2
        core = me % 2
        freq = ROPE_BASE ** (-jnp.arange(32, dtype=F32) / 32)
        angle = pre_len[0].astype(F32) * freq
        table = pre_table[0].T.astype(F32).reshape(4, 128)
        base = jnp.concatenate([jnp.tile(jnp.cos(angle), 2), jnp.tile(jnp.sin(angle), 2)])[None]
        wrow = jnp.broadcast_to(wr_table[0, 0, 0].astype(F32), (3, 128))
        meta = jnp.concatenate([table, base, wrow], axis=0)
        u, nk, lists, peer_c, peer_kr = project(
            hidden, meta, cos_i, sin_i, g_kv[None], w_q, w_dkv, w_uk.transpose(1, 2, 0), cache_c, cache_kr)
        offs = jnp.array([7, 6, 5, 3, 4, 2, 1, 0], jnp.int32)
        order = jnp.concatenate([chip ^ offs, jnp.stack([core, chip])]).astype(jnp.int32)
        part, c_out, kr_out = attend(lists, order, u, nk, w_uv.transpose(1, 0, 2), cache_c, cache_kr, peer_c, peer_kr)
        got = lax.all_to_all(part.reshape(DEVS, OUTR, 128), "pool", 0, 0, tiled=True)
        got = got.reshape(CHIPS, 2, OUTR, 128)
        o = got[:, :, :ROWS].reshape(CHIPS, DEVS, TOK, 128)
        m = got[:, :, ROWS:ROWS + 4].reshape(CHIPS, DEVS, TOK)
        l = got[:, :, ROWS + 4:].reshape(CHIPS, DEVS, TOK)
        w = jnp.exp2((m - jnp.max(m, axis=0, keepdims=True)) * EXP_SCALE)
        w = w / jnp.sum(w * l, axis=0, keepdims=True)
        o = jnp.sum(o * w[..., None], axis=0).astype(BF16)
        o = o.transpose(1, 0, 2).reshape(TOK, D_MODEL)
        y = hidden[0].astype(F32) + jnp.dot(o, w_o, preferred_element_type=F32)
        return y.astype(BF16)[None], c_out, kr_out

    row = P("pool")
    rep = P()
    return jax.shard_map(device_step, mesh=mesh, in_specs=(row,) * 6 + (rep,) * 6, out_specs=(row, row, row), check_vma=False)
```

```python
import functools
import math

import jax
import jax.numpy as jnp
import numpy as np
from jax import lax
from jax.experimental import pallas as pl
from jax.experimental.pallas import tpu as pltpu
from jax.sharding import PartitionSpec as P

MESH = pl.DeviceIdType.MESH
BF16 = jnp.bfloat16
F32 = jnp.float32

CHIPS = 8
DEVS = 16
TOK = 64
D_MODEL = 2048
HALF = 8
PAGE = 64
LAT = 512
ROPE = 64
NOPE = 128
KEYW = 640
ROWS = HALF * TOK
TABLE = 256
SLOTS = 64
OUTR = ROWS + 8
NORM_EPS = 1e-6
ROPE_BASE = 10000.0
EXP_SCALE = (NOPE + ROPE) ** -0.5 * math.log2(math.e)
NEG = -1e30
BLK_PAGES = 8
BLK = BLK_PAGES * PAGE


def xor3(a, b, bits):
    out = 0
    for i in range(bits):
        x = lax.rem(lax.div(a, 2**i), 2)
        y = lax.rem(lax.div(b, 2**i), 2) if not isinstance(b, int) else (b >> i) % 2
        out = out + 2**i * (x + y - 2 * x * y)
    return out


def project_kernel(
    x_hbm, meta_hbm, cos_ref, sin_ref, gkv_ref, wq_hbm, wdkv_hbm, wuk_hbm, wuv_hbm, cc_hbm, ckr_hbm,
    u_hbm, nk_hbm, list_ref, pc_hbm, pkr_hbm, wuvt_ref,
    xall, metas, wq, wdkv, wraw, wukt, ubuf, nkbuf,
    loc_sem, xs_sem, xr_sem, fs_sem, fr_sem, ms_sem, mr_sem, cs_sem, cr_sem, us_sem, ns_sem,
):
    me = lax.axis_index("pool")
    chip = lax.div(me, 2)
    core = lax.rem(me, 2)
    partner = me + 1 - 2 * core
    my_rows = pl.ds(pl.multiple_of(core * TOK, TOK), TOK)
    pt_rows = pl.ds(pl.multiple_of((1 - core) * TOK, TOK), TOK)

    x_in = pltpu.make_async_copy(x_hbm.at[0], xall.at[0, my_rows], loc_sem.at[0])
    x_in.start()
    m_in = pltpu.make_async_copy(meta_hbm, metas.at[me], loc_sem.at[1])
    m_in.start()
    wq_in = [
        pltpu.make_async_copy(
            wq_hbm.at[:, pl.ds(pl.multiple_of(core * (HALF * 192) + j * 384, 128), 384)],
            wq.at[j], loc_sem.at[2 + j])
        for j in range(4)
    ]
    half_heads = pl.ds(pl.multiple_of(core * HALF, HALF), HALF)
    wuk_in = pltpu.make_async_copy(wuk_hbm.at[:, half_heads], wraw.at[0], loc_sem.at[6])
    wuv_in = pltpu.make_async_copy(wuv_hbm.at[:, half_heads], wraw.at[1], loc_sem.at[8])
    wdkv_in = pltpu.make_async_copy(wdkv_hbm, wdkv, loc_sem.at[7])
    wdkv_in.start()
    for c in wq_in:
        c.start()
    wuk_in.start()
    wuv_in.start()

    barrier = pltpu.get_barrier_semaphore()
    for e in range(1, DEVS):
        pl.semaphore_signal(barrier, inc=1, device_id=(xor3(me, e, 4),), device_id_type=MESH)
    x_in.wait()
    m_in.wait()
    pl.semaphore_wait(barrier, DEVS - 1)

    x_own = xall.at[0, my_rows]
    sends = []
    for e in range(1, DEVS):
        sends.append(pltpu.make_async_remote_copy(
            src_ref=metas.at[me], dst_ref=metas.at[me], send_sem=ms_sem.at[e], recv_sem=mr_sem.at[e],
            device_id=(xor3(me, e, 4),), device_id_type=MESH))
    sends.append(pltpu.make_async_remote_copy(
        src_ref=x_own, dst_ref=x_own, send_sem=fs_sem.at[0], recv_sem=fr_sem.at[0],
        device_id=(partner,), device_id_type=MESH))
    for d in range(1, CHIPS):
        sends.append(pltpu.make_async_remote_copy(
            src_ref=x_own, dst_ref=xall.at[d, my_rows], send_sem=xs_sem.at[d], recv_sem=xr_sem.at[d],
            device_id=(2 * xor3(chip, d, 3) + core,), device_id_type=MESH))
    pc = pltpu.make_async_remote_copy(
        src_ref=cc_hbm.at[0, pl.ds(0, PAGE)], dst_ref=pc_hbm, send_sem=cs_sem.at[0], recv_sem=cr_sem.at[0],
        device_id=(partner,), device_id_type=MESH)
    pkr = pltpu.make_async_remote_copy(
        src_ref=ckr_hbm.at[0, pl.ds(0, PAGE)], dst_ref=pkr_hbm, send_sem=cs_sem.at[1], recv_sem=cr_sem.at[1],
        device_id=(partner,), device_id_type=MESH)
    sends += [pc, pkr]
    for s in sends:
        s.start()

    for e in range(1, DEVS):
        src = xor3(me, e, 4)
        pltpu.make_async_remote_copy(
            src_ref=metas.at[src], dst_ref=metas.at[src], send_sem=ms_sem.at[e], recv_sem=mr_sem.at[e],
            device_id=(src,), device_id_type=MESH).wait_recv()
    own = jnp.concatenate([metas[:, 0, :], metas[:, 1, :]], axis=1)
    page = jnp.concatenate([metas[:, 2, :], metas[:, 3, :]], axis=1)
    first = (2 * chip).astype(F32)
    mask = jnp.where(own >= first, 1.0, 0.0) * jnp.where(own < first + 2.0, 1.0, 0.0)
    tri_r = lax.broadcasted_iota(jnp.int32, (TABLE, TABLE), 0)
    tri_c = lax.broadcasted_iota(jnp.int32, (TABLE, TABLE), 1)
    tri = jnp.where(tri_r < tri_c, 1.0, 0.0).astype(BF16)
    rank = jnp.dot(mask.astype(BF16), tri, preferred_element_type=F32)
    rank = jnp.where(mask > 0.5, rank, -1.0)
    local = (own - first) * float(PAGE) + page
    lane = lax.broadcasted_iota(jnp.int32, (DEVS, 128), 1)
    count = jnp.sum(mask, axis=1, keepdims=True)
    req_id = lax.broadcasted_iota(jnp.int32, (DEVS, 1), 0).astype(F32)
    wr = jnp.sum(jnp.where(metas[:, 5, 0:1] == me.astype(F32), req_id, 0.0), axis=0, keepdims=True)
    base = jnp.where(lane == SLOTS, count, jnp.where(lane == SLOTS + 1, wr, 0.0))

    def slot(s, acc):
        hit = jnp.sum(jnp.where(rank == s.astype(F32), local, 0.0), axis=1, keepdims=True)
        return jnp.where(lane == s, hit, acc)

    list_ref[...] = lax.fori_loop(0, SLOTS, slot, base).astype(jnp.int32)

    wuk_in.wait()
    wuv_in.wait()
    wukt[...] = jnp.swapaxes(wraw[0], 0, 1)
    wuvt_ref[...] = jnp.swapaxes(wraw[1], 0, 1)

    lane2 = lax.broadcasted_iota(jnp.int32, (1, 128), 1)
    low = lane2 < 64
    first_half = lax.rem(lane2, 64) < 32
    wdkv_in.wait()
    for c in wq_in:
        c.wait()

    def rotate(v, cos_t, sin_t):
        turned = jnp.where(first_half, pltpu.roll(v, 96, 1), pltpu.roll(v, 32, 1))
        return v * cos_t + turned * sin_t

    def fwd(d, rows):
        ref = xall.at[d, rows]
        return pltpu.make_async_remote_copy(
            src_ref=ref, dst_ref=ref, send_sem=fs_sem.at[d], recv_sem=fr_sem.at[d],
            device_id=(partner,), device_id_type=MESH)

    def out_copies(slot_id, i):
        two = pl.ds(2 * i, 2)
        return (pltpu.make_async_copy(ubuf.at[slot_id], u_hbm.at[two], us_sem.at[slot_id]),
                pltpu.make_async_copy(nkbuf.at[slot_id], nk_hbm.at[two], ns_sem.at[slot_id]))

    def step(i, carry):
        slot_id = lax.rem(i, 2)
        for k in range(2):
            d = 2 * i + k

            @pl.when(d > 0)
            def _():
                ref = xall.at[d, my_rows]
                pltpu.make_async_remote_copy(
                    src_ref=ref, dst_ref=ref, send_sem=xs_sem.at[d], recv_sem=xr_sem.at[d],
                    device_id=(partner,), device_id_type=MESH).wait_recv()
                fwd(d, my_rows).start()

        for k in range(2):
            fwd(2 * i + k, pt_rows).wait_recv()

        @pl.when(i > 1)
        def _():
            for c in out_copies(slot_id, i):
                c.wait()

        cs, ss = [], []
        for k in range(2):
            src_chip = xor3(chip, 2 * i + k, 3)
            for half in range(2):
                b = metas[2 * src_chip + half, 4:5, :]
                br = pltpu.roll(b, 64, 1)
                cp = jnp.where(low, b, br)
                sp = jnp.where(low, br, b)
                cs.append(cp * cos_ref[...] - sp * sin_ref[...])
                ss.append((sp * cos_ref[...] + cp * sin_ref[...]) * jnp.where(first_half, -1.0, 1.0))
        cos_t = jnp.concatenate(cs, axis=0)
        sin_t = jnp.concatenate(ss, axis=0)

        def x_rows():
            return jnp.concatenate([xall[2 * i], xall[2 * i + 1]], axis=0)

        kv = lax.dot_general(x_rows(), wdkv[...], (((1,), (1,)), ((), ())), preferred_element_type=F32)
        lat = kv[:, :LAT]
        inv = lax.rsqrt(jnp.mean(lat * lat, axis=-1, keepdims=True) + NORM_EPS)
        c_new = (lat * inv * gkv_ref[...].astype(F32)).astype(BF16)
        kr = jnp.concatenate([kv[:, LAT:], jnp.zeros((4 * TOK, 64), F32)], axis=1)
        kr = rotate(kr, cos_t, sin_t).astype(BF16)
        for part in range(4):
            rows = slice(part * TOK, (part + 1) * TOK)
            nkbuf[slot_id, part // 2, part % 2, :, :LAT] = c_new[rows]
            nkbuf[slot_id, part // 2, part % 2, :, LAT:] = kr[rows]

        def pair(j, carry):
            q = jnp.dot(x_rows(), wq[j], preferred_element_type=F32).astype(BF16)
            nope = (q[:, 0:128], jnp.concatenate([q[:, 192:256], q[:, 256:320]], axis=1))
            rp = jnp.concatenate([q[:, 128:192], q[:, 320:384]], axis=1).astype(F32)
            rp = rotate(rp, cos_t, sin_t)
            rps = (jnp.where(low, rp, 0.0).astype(BF16), jnp.where(low, pltpu.roll(rp, 64, 1), 0.0).astype(BF16))
            for h in range(2):
                u = lax.dot_general(nope[h], wukt[2 * j + h], (((1,), (1,)), ((), ())), preferred_element_type=F32).astype(BF16)
                head_rows = pl.ds(pl.multiple_of((2 * j + h) * TOK, TOK), TOK)
                for part in range(4):
                    rows = slice(part * TOK, (part + 1) * TOK)
                    ubuf[slot_id, part // 2, part % 2, head_rows, :LAT] = u[rows]
                    ubuf[slot_id, part // 2, part % 2, head_rows, LAT:] = rps[h][rows]
            return carry

        lax.fori_loop(0, 4, pair, 0)
        for c in out_copies(slot_id, i):
            c.start()
        return carry

    lax.fori_loop(0, CHIPS // 2, step, 0)
    for slot_id in range(2):
        for c in out_copies(slot_id, slot_id):
            c.wait()
    for s in sends[:-2]:
        s.wait_send()
    for d in range(1, CHIPS):
        fwd(d, my_rows).wait_send()
    pc.wait()
    pkr.wait()


def project(x, meta, cos_i, sin_i, g_kv, w_q, w_dkvt, w_uk, w_uv, cache_c, cache_kr):
    any_spec = pl.BlockSpec(memory_space=pl.ANY)
    vmem = pl.BlockSpec(memory_space=pltpu.VMEM)
    dma = pltpu.SemaphoreType.DMA
    return pl.pallas_call(
        project_kernel,
        out_shape=(
            jax.ShapeDtypeStruct((CHIPS, 2, ROWS, KEYW), BF16),
            jax.ShapeDtypeStruct((CHIPS, 2, TOK, KEYW), BF16),
            jax.ShapeDtypeStruct((DEVS, 128), jnp.int32),
            jax.ShapeDtypeStruct((PAGE, PAGE, LAT), BF16),
            jax.ShapeDtypeStruct((PAGE, PAGE, ROPE), BF16),
            jax.ShapeDtypeStruct((HALF, LAT, NOPE), BF16),
        ),
        in_specs=[any_spec, any_spec, vmem, vmem, vmem] + [any_spec] * 6,
        out_specs=(any_spec, any_spec, vmem, any_spec, any_spec, vmem),
        scratch_shapes=[
            pltpu.VMEM((CHIPS, 2 * TOK, D_MODEL), BF16),
            pltpu.VMEM((DEVS, 8, 128), F32),
            pltpu.VMEM((4, D_MODEL, 384), BF16),
            pltpu.VMEM((LAT + ROPE, D_MODEL), BF16),
            pltpu.VMEM((2, LAT, HALF, NOPE), BF16),
            pltpu.VMEM((HALF, LAT, NOPE), BF16),
            pltpu.VMEM((2, 2, 2, ROWS, KEYW), BF16),
            pltpu.VMEM((2, 2, 2, TOK, KEYW), BF16),
            dma((9,)), dma((8,)), dma((8,)), dma((8,)), dma((8,)), dma((16,)), dma((16,)),
            dma((2,)), dma((2,)), dma((2,)), dma((2,)),
        ],
        compiler_params=pltpu.CompilerParams(collective_id=0, has_side_effects=True, vmem_limit_bytes=48 * 2**20),
        name="project",
    )(x, meta, cos_i, sin_i, g_kv, w_q, w_dkvt, w_uk, w_uv, cache_c, cache_kr)


def to_rows(col):
    lane = lax.broadcasted_iota(jnp.int32, (128, 128), 1)
    row = lax.broadcasted_iota(jnp.int32, (128, 128), 0)
    parts = [jnp.sum(jnp.where(lane == row, col[i * 128:(i + 1) * 128], 0.0), axis=0, keepdims=True) for i in range(4)]
    return jnp.concatenate(parts, axis=0)


def attend_kernel(
    list_ref, order_ref,
    u_ref, nk_hbm, wuv_ref, cc_hbm, ckr_hbm, pc_hbm, pkr_hbm,
    out_ref, occ_hbm, ockr_hbm,
    kv, krs, kg, s_buf, s_new, acc, lmax, lsum, nk_own, nk_wr, sem, osem,
):
    g = pl.program_id(0)
    core = order_ref[16]
    chip = order_ref[17]
    src_chip = order_ref[8 + g]
    own = pl.ds(pl.multiple_of(core * PAGE, PAGE), PAGE)
    oth = pl.ds(pl.multiple_of((1 - core) * PAGE, PAGE), PAGE)
    wr = list_ref[0, SLOTS + 1]

    outs = (
        pltpu.make_async_copy(kv.at[own, :, pl.ds(0, LAT)], occ_hbm.at[0, pl.ds(0, PAGE)], osem.at[0]),
        pltpu.make_async_copy(krs.at[own], ockr_hbm.at[0, pl.ds(0, PAGE)], osem.at[1]),
        pltpu.make_async_copy(nk_wr.at[:, pl.ds(0, LAT)], occ_hbm.at[0, PAGE], osem.at[2]),
        pltpu.make_async_copy(krs.at[2 * PAGE], ockr_hbm.at[0, PAGE], osem.at[3]),
    )

    @pl.when(g == 0)
    def _():
        ins = (
            pltpu.make_async_copy(ckr_hbm.at[0, pl.ds(0, PAGE)], krs.at[own], sem.at[0]),
            pltpu.make_async_copy(pkr_hbm, krs.at[oth], sem.at[1]),
            pltpu.make_async_copy(nk_hbm.at[order_ref[18 + lax.div(wr, 2)], lax.rem(wr, 2)], nk_wr, sem.at[2]),
            pltpu.make_async_copy(nk_hbm.at[0], nk_own.at[:, pl.ds(0, TOK)], sem.at[3]),
            pltpu.make_async_copy(cc_hbm.at[0, pl.ds(0, PAGE)], kv.at[own, :, pl.ds(0, LAT)], sem.at[4]),
            pltpu.make_async_copy(pc_hbm, kv.at[oth, :, pl.ds(0, LAT)], sem.at[5]),
        )
        for c in ins:
            c.start()
        for c in ins[:4]:
            c.wait()

        def fill(p, carry):
            kv[p, :, LAT:] = jnp.concatenate([krs[p], jnp.zeros((PAGE, 64), BF16)], axis=1)
            return carry

        lax.fori_loop(0, 2 * PAGE, fill, 0)
        krs[2 * PAGE] = nk_wr[:, LAT:LAT + ROPE]
        nk_own[:, TOK:, :] = jnp.zeros((2, TOK, KEYW), BF16)
        for c in ins[4:]:
            c.wait()
        for c in outs:
            c.start()

    nt = (((1,), (1,)), ((), ()))

    def lanes(op, v):
        out = v[:, 0:128]
        for i in range(1, v.shape[1] // 128):
            out = op(out, v[:, i * 128:(i + 1) * 128])
        return out

    for r in range(2):
        req = 2 * src_chip + r
        n = list_ref[req, SLOTS]
        blocks = lax.div(n + BLK_PAGES - 1, BLK_PAGES)
        acc[r] = jnp.zeros((ROWS, LAT), F32)
        lsum[...] = jnp.zeros_like(lsum)
        lmax[...] = jnp.full_like(lmax, NEG)

        def score(b, carry):
            keys = jnp.concatenate([kv[list_ref[req, b * BLK_PAGES + j]] for j in range(BLK_PAGES)], axis=0)
            kg[b] = keys[:, :LAT]
            s = lax.dot_general(u_ref[0, r], keys, nt, preferred_element_type=F32)
            key = b * BLK + lax.broadcasted_iota(jnp.int32, (1, BLK), 1)
            s = s + jnp.where(key < n * PAGE, 0.0, -jnp.inf)
            s_buf[b] = s
            lmax[...] = jnp.maximum(lmax[...], lanes(jnp.maximum, s))
            return carry

        lax.fori_loop(0, blocks, score, 0)

        @pl.when(src_chip == chip)
        def _():
            row = lax.rem(lax.broadcasted_iota(jnp.int32, (ROWS, 128), 0), TOK)
            key = lax.broadcasted_iota(jnp.int32, (ROWS, 128), 1)
            s = lax.dot_general(u_ref[0, r], nk_own[r], nt, preferred_element_type=F32)
            s = jnp.where(key <= row, s, -jnp.inf)
            s_new[...] = s
            lmax[...] = jnp.maximum(lmax[...], s)

        m = jnp.max(lmax[...], axis=1, keepdims=True)
        out_ref[0, r, ROWS:ROWS + 4, :] = to_rows(m)
        lmax[...] = jnp.broadcast_to(m * EXP_SCALE, lmax.shape)

        def gather_values(b, carry):
            mm = lmax[...]
            p = jnp.exp2(s_buf[b] * EXP_SCALE - jnp.concatenate([mm] * (BLK // 128), axis=1))
            lsum[...] += lanes(jnp.add, p)
            acc[r] += jnp.dot(p.astype(BF16), kg[b], preferred_element_type=F32)
            return carry

        lax.fori_loop(0, blocks, gather_values, 0)

        @pl.when(src_chip == chip)
        def _():
            p = jnp.exp2(s_new[...] * EXP_SCALE - lmax[...])
            lsum[...] += p
            acc[r] += jnp.dot(p.astype(BF16), nk_own[r, :, :LAT], preferred_element_type=F32)

        out_ref[0, r, ROWS + 4:, :] = to_rows(jnp.sum(lsum[...], axis=1, keepdims=True))

    for h in range(HALF):
        rows = slice(h * TOK, (h + 1) * TOK)
        terms = []
        for r in range(2):
            a = acc[r, rows, :]
            hi = a.astype(BF16)
            terms += [hi, (a - hi.astype(F32)).astype(BF16)]
        both = jnp.dot(jnp.concatenate(terms, axis=0), wuv_ref[h], preferred_element_type=F32)
        out_ref[0, 0, rows, :] = both[:TOK] + both[TOK:2 * TOK]
        out_ref[0, 1, rows, :] = both[2 * TOK:3 * TOK] + both[3 * TOK:]

    @pl.when(g == CHIPS - 1)
    def _():
        for c in outs:
            c.wait()


def attend(lists, order, u, nk, w_uvt, cache_c, cache_kr, peer_c, peer_kr):
    any_spec = pl.BlockSpec(memory_space=pl.ANY)
    dma = pltpu.SemaphoreType.DMA
    return pl.pallas_call(
        attend_kernel,
        grid_spec=pltpu.PrefetchScalarGridSpec(
            num_scalar_prefetch=2,
            grid=(CHIPS,),
            in_specs=[
                pl.BlockSpec((1, 2, ROWS, KEYW), lambda g, l, o: (o[g], 0, 0, 0)),
                any_spec,
                pl.BlockSpec(memory_space=pltpu.VMEM),
                any_spec, any_spec, any_spec, any_spec,
            ],
            out_specs=(
                pl.BlockSpec((1, 2, OUTR, 128), lambda g, l, o: (o[8 + g], 0, 0, 0)),
                any_spec, any_spec,
            ),
            scratch_shapes=[
                pltpu.VMEM((2 * PAGE, PAGE, KEYW), BF16),
                pltpu.VMEM((2 * PAGE + 1, PAGE, ROPE), BF16),
                pltpu.VMEM((SLOTS // BLK_PAGES, BLK, LAT), BF16),
                pltpu.VMEM((SLOTS // BLK_PAGES, ROWS, BLK), F32),
                pltpu.VMEM((ROWS, 128), F32),
                pltpu.VMEM((2, ROWS, LAT), F32),
                pltpu.VMEM((ROWS, 128), F32),
                pltpu.VMEM((ROWS, 128), F32),
                pltpu.VMEM((2, 2 * TOK, KEYW), BF16),
                pltpu.VMEM((TOK, KEYW), BF16),
                dma((6,)), dma((4,)),
            ],
        ),
        out_shape=(
            jax.ShapeDtypeStruct((CHIPS, 2, OUTR, 128), F32),
            jax.ShapeDtypeStruct(cache_c.shape, BF16),
            jax.ShapeDtypeStruct(cache_kr.shape, BF16),
        ),
        compiler_params=pltpu.CompilerParams(vmem_limit_bytes=56 * 2**20),
        name="attend",
    )(lists, order, u, nk, w_uvt, cache_c, cache_kr, peer_c, peer_kr)


def solution(mesh):
    tok_ids = np.arange(TOK, dtype=np.float64)[:, None]
    inv_freq = ROPE_BASE ** (-np.arange(32, dtype=np.float64) / 32)
    cos_i = np.tile(np.cos(tok_ids * inv_freq), (1, 4)).astype(np.float32)
    sin_i = np.tile(np.sin(tok_ids * inv_freq), (1, 4)).astype(np.float32)

    def device_step(hidden, pre_len, pre_table, wr_table, cache_c, cache_kr, w_q, w_dkv, g_kv, w_uk, w_uv, w_o):
        me = lax.axis_index("pool")
        chip = me // 2
        core = me % 2
        freq = ROPE_BASE ** (-jnp.arange(32, dtype=F32) / 32)
        angle = pre_len[0].astype(F32) * freq
        table = pre_table[0].T.astype(F32).reshape(4, 128)
        base = jnp.concatenate([jnp.tile(jnp.cos(angle), 2), jnp.tile(jnp.sin(angle), 2)])[None]
        wrow = jnp.broadcast_to(wr_table[0, 0, 0].astype(F32), (3, 128))
        meta = jnp.concatenate([table, base, wrow], axis=0)
        u, nk, lists, peer_c, peer_kr, w_uvt = project(
            hidden, meta, cos_i, sin_i, g_kv[None], w_q, w_dkv.T, w_uk, w_uv, cache_c, cache_kr)
        offs = jnp.array([7, 6, 5, 3, 4, 2, 1, 0], jnp.int32)
        order = jnp.concatenate([offs, chip ^ offs, jnp.stack([core, chip]), chip ^ jnp.arange(CHIPS)]).astype(jnp.int32)
        part, c_out, kr_out = attend(lists, order, u, nk, w_uvt, cache_c, cache_kr, peer_c, peer_kr)
        got = lax.all_to_all(part.reshape(DEVS, OUTR, 128), "pool", 0, 0, tiled=True)
        got = got.reshape(CHIPS, 2, OUTR, 128)
        o = got[:, :, :ROWS].reshape(CHIPS, DEVS, TOK, 128)
        m = got[:, :, ROWS:ROWS + 4].reshape(CHIPS, DEVS, TOK)
        l = got[:, :, ROWS + 4:].reshape(CHIPS, DEVS, TOK)
        w = jnp.exp2((m - jnp.max(m, axis=0, keepdims=True)) * EXP_SCALE)
        w = w / jnp.sum(w * l, axis=0, keepdims=True)
        o = jnp.sum(o * w[..., None], axis=0).astype(BF16)
        o = o.transpose(1, 0, 2).reshape(TOK, D_MODEL)
        y = hidden[0].astype(F32) + jnp.dot(o, w_o, preferred_element_type=F32)
        return y.astype(BF16)[None], c_out, kr_out

    row = P("pool")
    rep = P()
    return jax.shard_map(device_step, mesh=mesh, in_specs=(row,) * 6 + (rep,) * 6, out_specs=(row, row, row), check_vma=False)
```

```python
import functools
import math

import jax
import jax.numpy as jnp
import numpy as np
from jax import lax
from jax.experimental import pallas as pl
from jax.experimental.pallas import tpu as pltpu
from jax.sharding import PartitionSpec as P

MESH = pl.DeviceIdType.MESH
BF16 = jnp.bfloat16
F32 = jnp.float32

CHIPS = 8
DEVS = 16
TOK = 64
D_MODEL = 2048
HALF = 8
PAGE = 64
LAT = 512
ROPE = 64
NOPE = 128
KEYW = 640
ROWS = HALF * TOK
TABLE = 256
SLOTS = 64
OUTR = ROWS + 8
NORM_EPS = 1e-6
ROPE_BASE = 10000.0
EXP_SCALE = (NOPE + ROPE) ** -0.5 * math.log2(math.e)
NEG = -1e30
BLK_PAGES = 8
BLK = BLK_PAGES * PAGE


def xor3(a, b, bits):
    out = 0
    for i in range(bits):
        x = lax.rem(lax.div(a, 2**i), 2)
        y = lax.rem(lax.div(b, 2**i), 2) if not isinstance(b, int) else (b >> i) % 2
        out = out + 2**i * (x + y - 2 * x * y)
    return out


def project_kernel(
    x_hbm, meta_hbm, cos_ref, sin_ref, gkv_ref, wq_hbm, wdkv_hbm, wuk_hbm, wuv_hbm, cc_hbm, ckr_hbm,
    u_hbm, nk_hbm, list_ref, kv, wuvt_ref,
    xall, metas, krs, wq, wdkv, wraw, wukt, ubuf, nkbuf,
    loc_sem, xs_sem, xr_sem, fs_sem, fr_sem, ms_sem, mr_sem, cs_sem, cr_sem, us_sem, ns_sem,
):
    me = lax.axis_index("pool")
    chip = lax.div(me, 2)
    core = lax.rem(me, 2)
    partner = me + 1 - 2 * core
    my_rows = pl.ds(pl.multiple_of(core * TOK, TOK), TOK)
    pt_rows = pl.ds(pl.multiple_of((1 - core) * TOK, TOK), TOK)

    x_in = pltpu.make_async_copy(x_hbm.at[0], xall.at[0, my_rows], loc_sem.at[0])
    x_in.start()
    m_in = pltpu.make_async_copy(meta_hbm, metas.at[me], loc_sem.at[1])
    m_in.start()
    wq_in = [
        pltpu.make_async_copy(
            wq_hbm.at[:, pl.ds(pl.multiple_of(core * (HALF * 192) + j * 768, 128), 768)],
            wq.at[j], loc_sem.at[2 + j])
        for j in range(2)
    ]
    half_heads = pl.ds(pl.multiple_of(core * HALF, HALF), HALF)
    wuk_in = pltpu.make_async_copy(wuk_hbm.at[:, half_heads], wraw.at[0], loc_sem.at[6])
    wuv_in = pltpu.make_async_copy(wuv_hbm.at[:, half_heads], wraw.at[1], loc_sem.at[8])
    wdkv_in = pltpu.make_async_copy(wdkv_hbm, wdkv, loc_sem.at[7])
    wdkv_in.start()
    for c in wq_in:
        c.start()
    wuk_in.start()
    wuv_in.start()

    barrier = pltpu.get_barrier_semaphore()
    for e in range(1, DEVS):
        pl.semaphore_signal(barrier, inc=1, device_id=(xor3(me, e, 4),), device_id_type=MESH)
    x_in.wait()
    m_in.wait()
    pl.semaphore_wait(barrier, DEVS - 1)

    x_own = xall.at[0, my_rows]
    sends = []
    for e in range(1, DEVS):
        sends.append(pltpu.make_async_remote_copy(
            src_ref=metas.at[me], dst_ref=metas.at[me], send_sem=ms_sem.at[e], recv_sem=mr_sem.at[e],
            device_id=(xor3(me, e, 4),), device_id_type=MESH))
    sends.append(pltpu.make_async_remote_copy(
        src_ref=x_own, dst_ref=x_own, send_sem=fs_sem.at[0], recv_sem=fr_sem.at[0],
        device_id=(partner,), device_id_type=MESH))
    for d in range(1, CHIPS):
        sends.append(pltpu.make_async_remote_copy(
            src_ref=x_own, dst_ref=xall.at[d, my_rows], send_sem=xs_sem.at[d], recv_sem=xr_sem.at[d],
            device_id=(2 * xor3(chip, d, 3) + core,), device_id_type=MESH))
    own_pages = pl.ds(pl.multiple_of(core * PAGE, PAGE), PAGE)
    oth_pages = pl.ds(pl.multiple_of((1 - core) * PAGE, PAGE), PAGE)
    lat_cols = pl.ds(0, LAT)
    own_c, own_kr = cc_hbm.at[0, pl.ds(0, PAGE)], ckr_hbm.at[0, pl.ds(0, PAGE)]
    kv_in = [
        pltpu.make_async_copy(own_c, kv.at[own_pages, :, lat_cols], loc_sem.at[9]),
        pltpu.make_async_copy(own_kr, krs.at[own_pages], loc_sem.at[10]),
    ]
    sends += [
        pltpu.make_async_remote_copy(
            src_ref=own_c, dst_ref=kv.at[own_pages, :, lat_cols], send_sem=cs_sem.at[0], recv_sem=cr_sem.at[0],
            device_id=(partner,), device_id_type=MESH),
        pltpu.make_async_remote_copy(
            src_ref=own_kr, dst_ref=krs.at[own_pages], send_sem=cs_sem.at[1], recv_sem=cr_sem.at[1],
            device_id=(partner,), device_id_type=MESH),
    ]
    for s in sends:
        s.start()
    for c in kv_in:
        c.start()

    for e in range(1, DEVS):
        src = xor3(me, e, 4)
        pltpu.make_async_remote_copy(
            src_ref=metas.at[src], dst_ref=metas.at[src], send_sem=ms_sem.at[e], recv_sem=mr_sem.at[e],
            device_id=(src,), device_id_type=MESH).wait_recv()
    own = jnp.concatenate([metas[:, 0, :], metas[:, 1, :]], axis=1)
    page = jnp.concatenate([metas[:, 2, :], metas[:, 3, :]], axis=1)
    first = (2 * chip).astype(F32)
    mask = jnp.where(own >= first, 1.0, 0.0) * jnp.where(own < first + 2.0, 1.0, 0.0)
    tri_r = lax.broadcasted_iota(jnp.int32, (TABLE, TABLE), 0)
    tri_c = lax.broadcasted_iota(jnp.int32, (TABLE, TABLE), 1)
    tri = jnp.where(tri_r < tri_c, 1.0, 0.0).astype(BF16)
    rank = jnp.dot(mask.astype(BF16), tri, preferred_element_type=F32)
    rank = jnp.where(mask > 0.5, rank, -1.0)
    local = (own - first) * float(PAGE) + page
    lane = lax.broadcasted_iota(jnp.int32, (DEVS, 128), 1)
    count = jnp.sum(mask, axis=1, keepdims=True)
    req_id = lax.broadcasted_iota(jnp.int32, (DEVS, 1), 0).astype(F32)
    wr = jnp.sum(jnp.where(metas[:, 5, 0:1] == me.astype(F32), req_id, 0.0), axis=0, keepdims=True)
    base = jnp.where(lane == SLOTS, count, jnp.where(lane == SLOTS + 1, wr, 0.0))

    def slots(t, acc):
        for k in range(16):
            s = t * 16 + k
            hit = jnp.sum(jnp.where(rank == s.astype(F32), local, 0.0), axis=1, keepdims=True)
            acc = jnp.where(lane == s, hit, acc)
        return acc

    list_ref[...] = lax.fori_loop(0, SLOTS // 16, slots, base).astype(jnp.int32)

    wuk_in.wait()
    wuv_in.wait()
    wukt[...] = jnp.swapaxes(wraw[0], 0, 1)
    wuvt_ref[...] = jnp.swapaxes(wraw[1], 0, 1)

    lane2 = lax.broadcasted_iota(jnp.int32, (1, 128), 1)
    low = lane2 < 64
    first_half = lax.rem(lane2, 64) < 32
    wdkv_in.wait()
    for c in wq_in:
        c.wait()

    def rotate(v, cos_t, sin_t):
        turned = jnp.where(first_half, pltpu.roll(v, 96, 1), pltpu.roll(v, 32, 1))
        return v * cos_t + turned * sin_t

    def fwd(d, rows):
        ref = xall.at[d, rows]
        return pltpu.make_async_remote_copy(
            src_ref=ref, dst_ref=ref, send_sem=fs_sem.at[d], recv_sem=fr_sem.at[d],
            device_id=(partner,), device_id_type=MESH)

    def out_copies(slot_id, i):
        two = pl.ds(2 * i, 2)
        return (pltpu.make_async_copy(ubuf.at[slot_id], u_hbm.at[two], us_sem.at[slot_id]),
                pltpu.make_async_copy(nkbuf.at[slot_id], nk_hbm.at[two], ns_sem.at[slot_id]))

    def step(i, carry):
        slot_id = lax.rem(i, 2)
        for k in range(2):
            d = 2 * i + k

            @pl.when(d > 0)
            def _():
                ref = xall.at[d, my_rows]
                pltpu.make_async_remote_copy(
                    src_ref=ref, dst_ref=ref, send_sem=xs_sem.at[d], recv_sem=xr_sem.at[d],
                    device_id=(partner,), device_id_type=MESH).wait_recv()
                fwd(d, my_rows).start()

        for k in range(2):
            fwd(2 * i + k, pt_rows).wait_recv()

        @pl.when(i > 1)
        def _():
            for c in out_copies(slot_id, i):
                c.wait()

        cs, ss = [], []
        for k in range(2):
            src_chip = xor3(chip, 2 * i + k, 3)
            for half in range(2):
                b = metas[2 * src_chip + half, 4:5, :]
                br = pltpu.roll(b, 64, 1)
                cp = jnp.where(low, b, br)
                sp = jnp.where(low, br, b)
                cs.append(cp * cos_ref[...] - sp * sin_ref[...])
                ss.append((sp * cos_ref[...] + cp * sin_ref[...]) * jnp.where(first_half, -1.0, 1.0))
        cos_t = jnp.concatenate(cs, axis=0)
        sin_t = jnp.concatenate(ss, axis=0)

        def x_rows():
            return jnp.concatenate([xall[2 * i], xall[2 * i + 1]], axis=0)

        kv = lax.dot_general(x_rows(), wdkv[...], (((1,), (1,)), ((), ())), preferred_element_type=F32)
        lat = kv[:, :LAT]
        inv = lax.rsqrt(jnp.mean(lat * lat, axis=-1, keepdims=True) + NORM_EPS)
        c_new = (lat * inv * gkv_ref[...].astype(F32)).astype(BF16)
        kr = jnp.concatenate([kv[:, LAT:], jnp.zeros((4 * TOK, 64), F32)], axis=1)
        kr = rotate(kr, cos_t, sin_t).astype(BF16)
        for part in range(4):
            rows = slice(part * TOK, (part + 1) * TOK)
            nkbuf[slot_id, part // 2, part % 2, :, :LAT] = c_new[rows]
            nkbuf[slot_id, part // 2, part % 2, :, LAT:] = kr[rows]

        def four(j, carry):
            q = jnp.dot(x_rows(), wq[j], preferred_element_type=F32).astype(BF16)
            for t in range(2):
                o = t * 384
                nope = (q[:, o:o + 128], jnp.concatenate([q[:, o + 192:o + 256], q[:, o + 256:o + 320]], axis=1))
                rp = jnp.concatenate([q[:, o + 128:o + 192], q[:, o + 320:o + 384]], axis=1).astype(F32)
                rp = rotate(rp, cos_t, sin_t)
                rps = (jnp.where(low, rp, 0.0).astype(BF16), jnp.where(low, pltpu.roll(rp, 64, 1), 0.0).astype(BF16))
                for h in range(2):
                    head = 4 * j + 2 * t + h
                    u = lax.dot_general(nope[h], wukt[head], (((1,), (1,)), ((), ())), preferred_element_type=F32).astype(BF16)
                    head_rows = pl.ds(pl.multiple_of(head * TOK, TOK), TOK)
                    for part in range(4):
                        rows = slice(part * TOK, (part + 1) * TOK)
                        ubuf[slot_id, part // 2, part % 2, head_rows, :LAT] = u[rows]
                        ubuf[slot_id, part // 2, part % 2, head_rows, LAT:] = rps[h][rows]
            return carry

        lax.fori_loop(0, 2, four, 0)
        for c in out_copies(slot_id, i):
            c.start()
        return carry

    lax.fori_loop(0, CHIPS // 2, step, 0)

    def fill(p, carry):
        kv[p, :, LAT:] = jnp.concatenate([krs[p], jnp.zeros((PAGE, 64), BF16)], axis=1)
        return carry

    kv_in[1].wait()
    sends[-1].wait()
    lax.fori_loop(0, 2 * PAGE, fill, 0, unroll=8)
    kv_in[0].wait()
    sends[-2].wait()
    for slot_id in range(2):
        for c in out_copies(slot_id, slot_id):
            c.wait()
    for s in sends[:-2]:
        s.wait_send()
    for d in range(1, CHIPS):
        fwd(d, my_rows).wait_send()


def project(x, meta, cos_i, sin_i, g_kv, w_q, w_dkvt, w_uk, w_uv, cache_c, cache_kr):
    any_spec = pl.BlockSpec(memory_space=pl.ANY)
    vmem = pl.BlockSpec(memory_space=pltpu.VMEM)
    dma = pltpu.SemaphoreType.DMA
    return pl.pallas_call(
        project_kernel,
        out_shape=(
            jax.ShapeDtypeStruct((CHIPS, 2, ROWS, KEYW), BF16),
            jax.ShapeDtypeStruct((CHIPS, 2, TOK, KEYW), BF16),
            jax.ShapeDtypeStruct((DEVS, 128), jnp.int32),
            jax.ShapeDtypeStruct((2 * PAGE, PAGE, KEYW), BF16),
            jax.ShapeDtypeStruct((HALF, LAT, NOPE), BF16),
        ),
        in_specs=[any_spec, any_spec, vmem, vmem, vmem] + [any_spec] * 6,
        out_specs=(any_spec, any_spec, vmem, vmem, vmem),
        scratch_shapes=[
            pltpu.VMEM((CHIPS, 2 * TOK, D_MODEL), BF16),
            pltpu.VMEM((DEVS, 8, 128), F32),
            pltpu.VMEM((2 * PAGE, PAGE, ROPE), BF16),
            pltpu.VMEM((2, D_MODEL, 768), BF16),
            pltpu.VMEM((LAT + ROPE, D_MODEL), BF16),
            pltpu.VMEM((2, LAT, HALF, NOPE), BF16),
            pltpu.VMEM((HALF, LAT, NOPE), BF16),
            pltpu.VMEM((2, 2, 2, ROWS, KEYW), BF16),
            pltpu.VMEM((2, 2, 2, TOK, KEYW), BF16),
            dma((11,)), dma((8,)), dma((8,)), dma((8,)), dma((8,)), dma((16,)), dma((16,)),
            dma((2,)), dma((2,)), dma((2,)), dma((2,)),
        ],
        compiler_params=pltpu.CompilerParams(collective_id=0, has_side_effects=True, vmem_limit_bytes=48 * 2**20),
        name="project",
    )(x, meta, cos_i, sin_i, g_kv, w_q, w_dkvt, w_uk, w_uv, cache_c, cache_kr)


def to_rows(col):
    lane = lax.broadcasted_iota(jnp.int32, (128, 128), 1)
    row = lax.broadcasted_iota(jnp.int32, (128, 128), 0)
    parts = [jnp.sum(jnp.where(lane == row, col[i * 128:(i + 1) * 128], 0.0), axis=0, keepdims=True) for i in range(4)]
    return jnp.concatenate(parts, axis=0)


def attend_kernel(group, writes, list_ref, order_ref, u_ref, kv, wuv_ref, *refs):
    refs = list(refs)
    nd = len(group)
    has_own = 0 in group
    nk_own = refs.pop(0) if has_own else None
    if writes:
        nk_hbm, ckr_hbm = refs.pop(0), refs.pop(0)
    part_refs = [refs.pop(0) for _ in range(2 * nd)]
    if writes:
        occ_hbm, ockr_hbm = refs.pop(0), refs.pop(0)
    kg, s_buf, s_new, acc, lmax, lsum, stage, psem = refs[:8]
    g = pl.program_id(0)
    core = order_ref[8]
    src_chip = order_ref[9]
    for i, d in enumerate(group):
        src_chip = jnp.where(g == i, order_ref[d], src_chip)

    if writes:
        krs, nk_wr, sem, osem = refs[8:]
        wr = list_ref[0, SLOTS + 1]
        own = pl.ds(pl.multiple_of(core * PAGE, PAGE), PAGE)
        outs = (
            pltpu.make_async_copy(kv.at[own, :, pl.ds(0, LAT)], occ_hbm.at[0, pl.ds(0, PAGE)], osem.at[0]),
            pltpu.make_async_copy(nk_wr.at[:, pl.ds(0, LAT)], occ_hbm.at[0, PAGE], osem.at[1]),
            pltpu.make_async_copy(krs, ockr_hbm, osem.at[2]),
        )
        ins = (
            pltpu.make_async_copy(ckr_hbm, krs, sem.at[0]),
            pltpu.make_async_copy(nk_hbm.at[order_ref[10 + lax.div(wr, 2)], lax.rem(wr, 2)], nk_wr, sem.at[1]),
        )

        @pl.when(g == 0)
        def _():
            outs[0].start()
            for c in ins:
                c.start()

        @pl.when(g == nd - 1)
        def _():
            for c in ins:
                c.wait()
            krs[0, PAGE] = nk_wr[:, LAT:LAT + ROPE]
            for c in outs[1:]:
                c.start()

    nt = (((1,), (1,)), ((), ()))

    def lanes(op, v):
        out = v[:, 0:128]
        for i in range(1, v.shape[1] // 128):
            out = op(out, v[:, i * 128:(i + 1) * 128])
        return out

    for b in range(2):
        r = core + b - 2 * core * b
        req = 2 * src_chip + r
        n = list_ref[req, SLOTS]
        blocks = lax.div(n + BLK_PAGES - 1, BLK_PAGES)
        acc[b] = jnp.zeros((ROWS, LAT), F32)
        lsum[...] = jnp.zeros_like(lsum)
        lmax[...] = jnp.full_like(lmax, NEG)

        def score(t, carry):
            keys = jnp.concatenate([kv[list_ref[req, t * BLK_PAGES + j]] for j in range(BLK_PAGES)], axis=0)
            kg[t] = keys[:, :LAT]
            s = lax.dot_general(u_ref[0, r], keys, nt, preferred_element_type=F32)
            key = t * BLK + lax.broadcasted_iota(jnp.int32, (1, BLK), 1)
            s = s + jnp.where(key < n * PAGE, 0.0, -jnp.inf)
            s_buf[t] = s
            lmax[...] = jnp.maximum(lmax[...], lanes(jnp.maximum, s))
            return carry

        lax.fori_loop(0, blocks, score, 0)

        if has_own:
            @pl.when(src_chip == order_ref[9])
            def _():
                row = lax.rem(lax.broadcasted_iota(jnp.int32, (ROWS, TOK), 0), TOK)
                key = lax.broadcasted_iota(jnp.int32, (ROWS, TOK), 1)
                s = lax.dot_general(u_ref[0, r], nk_own[0, r], nt, preferred_element_type=F32)
                s = jnp.where(key <= row, s, -jnp.inf)
                s_new[...] = jnp.concatenate([s, jnp.full((ROWS, 128 - TOK), -jnp.inf, F32)], axis=1)
                lmax[...] = jnp.maximum(lmax[...], s_new[...])

        m = jnp.max(lmax[...], axis=1, keepdims=True)
        stage[g, b, ROWS:ROWS + 4, :] = to_rows(m)
        lmax[...] = jnp.broadcast_to(m * EXP_SCALE, lmax.shape)

        def values(t, carry):
            mm = lmax[...]
            p = jnp.exp2(s_buf[t] * EXP_SCALE - jnp.concatenate([mm] * (BLK // 128), axis=1))
            lsum[...] += lanes(jnp.add, p)
            acc[b] += jnp.dot(p.astype(BF16), kg[t], preferred_element_type=F32)
            return carry

        lax.fori_loop(0, blocks, values, 0)

        if has_own:
            @pl.when(src_chip == order_ref[9])
            def _():
                p = jnp.exp2(s_new[...] * EXP_SCALE - lmax[...])
                lsum[...] += p
                acc[b] += jnp.dot(p[:, :TOK].astype(BF16), nk_own[0, r, :, :LAT], preferred_element_type=F32)

        stage[g, b, ROWS + 4:, :] = to_rows(jnp.sum(lsum[...], axis=1, keepdims=True))

    for h in range(HALF):
        rows = slice(h * TOK, (h + 1) * TOK)
        terms = []
        for b in range(2):
            a = acc[b, rows, :]
            hi = a.astype(BF16)
            terms += [hi, (a - hi.astype(F32)).astype(BF16)]
        both = jnp.dot(jnp.concatenate(terms, axis=0), wuv_ref[h], preferred_element_type=F32)
        stage[g, 0, rows, :] = both[:TOK] + both[TOK:2 * TOK]
        stage[g, 1, rows, :] = both[2 * TOK:3 * TOK] + both[3 * TOK:]

    def part_copy(i, b):
        return pltpu.make_async_copy(stage.at[i, b], part_refs[2 * i + b], psem.at[i, b])

    for i in range(nd):
        @pl.when(g == i)
        def _():
            for b in range(2):
                part_copy(i, b).start()

    @pl.when(g == nd - 1)
    def _():
        for i in range(nd):
            for b in range(2):
                part_copy(i, b).wait()
        if writes:
            for c in outs:
                c.wait()


def attend(group, lists, order, u, kv, w_uvt, nk, cache_c=None, cache_kr=None):
    any_spec = pl.BlockSpec(memory_space=pl.ANY)
    vmem = pl.BlockSpec(memory_space=pltpu.VMEM)
    dma = pltpu.SemaphoreType.DMA
    nd = len(group)
    has_own = 0 in group
    writes = cache_c is not None
    first = 18 + len(sum(GROUPS[:GROUPS.index(group)], ()))
    ops = [u, kv, w_uvt]
    in_specs = [pl.BlockSpec((1, 2, ROWS, KEYW), lambda g, l, o: (o[first + g], 0, 0, 0)), vmem, vmem]
    out_shape = [jax.ShapeDtypeStruct((OUTR, 128), F32)] * (2 * nd)
    scratch = [
        pltpu.VMEM((SLOTS // BLK_PAGES, BLK, LAT), BF16),
        pltpu.VMEM((SLOTS // BLK_PAGES, ROWS, BLK), F32),
        pltpu.VMEM((ROWS, 128), F32),
        pltpu.VMEM((2, ROWS, LAT), F32),
        pltpu.VMEM((ROWS, 128), F32),
        pltpu.VMEM((ROWS, 128), F32),
        pltpu.VMEM((nd, 2, OUTR, 128), F32),
        dma((nd, 2)),
    ]
    if has_own:
        ops.append(nk)
        in_specs.append(pl.BlockSpec((1, 2, TOK, KEYW), lambda g, l, o: (0, 0, 0, 0)))
    if writes:
        ops += [nk, cache_kr]
        in_specs += [any_spec, any_spec]
        out_shape += [jax.ShapeDtypeStruct(cache_c.shape, BF16), jax.ShapeDtypeStruct(cache_kr.shape, BF16)]
        scratch += [pltpu.VMEM((1, PAGE + 1, PAGE, ROPE), BF16), pltpu.VMEM((TOK, KEYW), BF16), dma((2,)), dma((3,))]
    return pl.pallas_call(
        functools.partial(attend_kernel, group, writes),
        grid_spec=pltpu.PrefetchScalarGridSpec(
            num_scalar_prefetch=2, grid=(nd,), in_specs=in_specs,
            out_specs=[any_spec] * len(out_shape), scratch_shapes=scratch,
        ),
        out_shape=out_shape,
        cost_estimate=pl.CostEstimate(flops=nd * 8 * 10**9, bytes_accessed=nd * 4 * 10**6, transcendentals=0),
        compiler_params=pltpu.CompilerParams(vmem_limit_bytes=34 * 2**20),
        name=f"attend_{group[0]}",
    )(lists, order, *ops)


def finish_kernel(order_ref, x_ref, wo_ref, *refs):
    parts, y_ref = refs[:16], refs[16]
    core = order_ref[8]
    total = x_ref[0].astype(F32)
    for b in range(2):
        mine = parts[8 * b:8 * b + 8]
        ms = [p[ROWS:ROWS + 4, :] for p in mine]
        top = functools.reduce(jnp.maximum, ms)
        ws = [jnp.exp2((m - top) * EXP_SCALE) for m in ms]
        den = functools.reduce(jnp.add, [w * p[ROWS + 4:, :] for w, p in zip(ws, mine)])
        fs = [w / den for w in ws]
        heads = []
        for i in range(4):
            cols = jnp.concatenate([f[i:i + 1] for f in fs], axis=0).T
            rows = slice(i * 128, (i + 1) * 128)
            o = functools.reduce(jnp.add, [p[rows, :] * cols[:, d:d + 1] for d, p in enumerate(mine)]).astype(BF16)
            heads += [o[:TOK], o[TOK:]]
        half = core + b - 2 * core * b
        w = wo_ref[pl.ds(pl.multiple_of(half * 1024, 1024), 1024), :]
        total = total + jnp.dot(jnp.concatenate(heads, axis=1), w, preferred_element_type=F32)
    y_ref[0] = total.astype(BF16)


def finish(order, x, w_o, parts):
    vmem = pl.BlockSpec(memory_space=pltpu.VMEM)
    return pl.pallas_call(
        finish_kernel,
        out_shape=jax.ShapeDtypeStruct(x.shape, BF16),
        in_specs=[pl.BlockSpec(memory_space=pltpu.SMEM)] + [vmem] * 18,
        out_specs=vmem,
        compiler_params=pltpu.CompilerParams(vmem_limit_bytes=30 * 2**20),
        cost_estimate=pl.CostEstimate(flops=10**9, bytes_accessed=13 * 10**6, transcendentals=0),
        name="finish",
    )(order, x, w_o, *parts)


GROUPS = ((7, 6), (5, 3), (4, 2, 1), (0,))


def solution(mesh):
    tok_ids = np.arange(TOK, dtype=np.float64)[:, None]
    inv_freq = ROPE_BASE ** (-np.arange(32, dtype=np.float64) / 32)
    cos_i = np.tile(np.cos(tok_ids * inv_freq), (1, 4)).astype(np.float32)
    sin_i = np.tile(np.sin(tok_ids * inv_freq), (1, 4)).astype(np.float32)

    def device_step(hidden, pre_len, pre_table, wr_table, cache_c, cache_kr, w_q, w_dkv, g_kv, w_uk, w_uv, w_o):
        me = lax.axis_index("pool")
        chip = me // 2
        core = me % 2
        freq = ROPE_BASE ** (-jnp.arange(32, dtype=F32) / 32)
        angle = pre_len[0].astype(F32) * freq
        table = pre_table[0].T.astype(F32).reshape(4, 128)
        base = jnp.concatenate([jnp.tile(jnp.cos(angle), 2), jnp.tile(jnp.sin(angle), 2)])[None]
        wrow = jnp.broadcast_to(wr_table[0, 0, 0].astype(F32), (3, 128))
        meta = jnp.concatenate([table, base, wrow], axis=0)
        u, nk, lists, kv, w_uvt = project(
            hidden, meta, cos_i, sin_i, g_kv[None], w_q, w_dkv.T, w_uk, w_uv, cache_c, cache_kr)
        near = chip ^ jnp.arange(CHIPS)
        order = jnp.concatenate([near, jnp.stack([core, chip]), near, jnp.array(sum(GROUPS, ()))]).astype(jnp.int32)
        parts = [[None] * CHIPS for _ in range(2)]
        for group in GROUPS:
            if group is GROUPS[0]:
                *mine, c_out, kr_out = attend(group, lists, order, u, kv, w_uvt, nk, cache_c, cache_kr)
            else:
                mine = attend(group, lists, order, u, kv, w_uvt, nk)
            for i, d in enumerate(group):
                for b in range(2):
                    part = mine[2 * i + b]
                    if d or b:
                        part = lax.ppermute(part, "pool", [(p, p ^ (2 * d + b)) for p in range(DEVS)])
                    parts[b][d] = part
        y = finish(order, hidden, w_o, parts[0] + parts[1])
        return y, c_out, kr_out

    row = P("pool")
    rep = P()
    return jax.shard_map(device_step, mesh=mesh, in_specs=(row,) * 6 + (rep,) * 6, out_specs=(row, row, row), check_vma=False)
```
